32 devices in a mesh: dp: 16 (over z, y, core), chan: 2 (over x).
Axes of the slice: x: 2, y: 2, z: 4, core: 2. Of those that a mesh axis runs over, the one named last changes fastest.
Arguments:
- inputs: bfloat16 [768, 196, 1024], P('dp', None, 'chan'), may hold values from -6 to 6
- norm_gain: float32 [1024], P('chan'), may hold values from 0.5 to 1.5
- norm_bias: float32 [1024], P('chan'), may hold values from -3 to 3
- w_first: bfloat16 [512, 196], replicated, may hold values from -0.4375 to 0.4375
- b_first: float32 [512], replicated, may hold values from -3 to 3
- w_second: bfloat16 [196, 512], replicated, may hold values from -0.25 to 0.25
- upstream: bfloat16 [768, 196, 1024], P('dp', None, 'chan'), may hold values from -6 to 6
Outputs:
- grad_input: bfloat16 [768, 196, 1024], P('dp', None, 'chan')
- grad_first: float32 [512, 196], P('dp')
- grad_second: float32 [196, 512], P(None, 'dp')
- grad_bias_first: float32 [512], P('dp')
- grad_gain: float32 [1024], P('chan')
- grad_shift: float32 [1024], P('chan')
The draws below stay inside these ranges and needn't reach their ends.
All inputs are finite; a program needn't handle non-finite values.
Results may differ from the reference program's by a relative error of at most 0.0056.
Values sent between devices are 32-bit elements; how exact they have to be, the bound alone decides.
No kernel may reach another device: no remote copies, remote signals or barrier semaphores. Data moves between devices by JAX's collectives and lax.ppermute only.
A program may use at most 192 MiB of HBM per device.

```python
import jax
import jax.numpy as jnp
from jax import lax

D = 1024
PATCHES = 196
TOKEN_HIDDEN = 512
B_DEV = 48
BATCH = 768
N_DP = 16


def shard_levels(key, shape, pieces, low, high):
    factor_of = 1.0
    for axis_at, shards_of in pieces:
        heights = jax.random.uniform(jax.random.fold_in(jax.random.fold_in(key, 6), axis_at), (shards_of,), jnp.float32, low / len(pieces), high / len(pieces))
        factor_of = factor_of * jnp.repeat(jnp.exp(heights), shape[axis_at] // shards_of).reshape((-1,) + (1,) * (len(shape) - 1 - axis_at))
    return factor_of


def centred(rng, shape, spread, limit, shards=(), held_as=jnp.bfloat16):
    level = shard_levels(rng, shape, shards, -0.22, 0.18) if shards else 1.0
    array = jax.random.normal(rng, shape, jnp.float32) * spread * level
    return jnp.minimum(jnp.maximum(array, -limit), limit).astype(held_as)


def setup_inputs(seed: int = 0) -> dict:
    arg_keys = jax.random.split(jax.random.key(seed), 8)
    inputs = centred(arg_keys[0], (BATCH, PATCHES, D), 1.0, 6.0, ((0, 16), (2, 2)))
    norm_gain = jnp.clip(1.0 + 0.1 * jax.random.normal(arg_keys[1], (D,), jnp.float32), 0.5, 1.5)
    norm_bias = centred(arg_keys[2], (D,), 0.5, 3.0, ((0, 2),), jnp.float32)
    w_first = centred(arg_keys[3], (TOKEN_HIDDEN, PATCHES), PATCHES ** -0.5, 0.4375)
    b_first = centred(arg_keys[4], (TOKEN_HIDDEN,), 0.5, 3.0, (), jnp.float32)
    w_second = centred(arg_keys[5], (PATCHES, TOKEN_HIDDEN), TOKEN_HIDDEN ** -0.5, 0.25)
    upstream = centred(arg_keys[6], (BATCH, PATCHES, D), 1.0, 6.0, ((0, 16), (2, 2)))
    return dict(inputs=inputs, norm_gain=norm_gain, norm_bias=norm_bias, w_first=w_first, b_first=b_first, w_second=w_second, upstream=upstream)


epsilon = 1e-06

def block_pass(values_in, upstream, norm_gain, norm_bias, w_first, b_first, w_second):
    values = values_in.astype(jnp.float32)
    row_mean = lax.optimization_barrier(jnp.mean(values, axis=-1, keepdims=True))
    centered = values - row_mean
    row_var = lax.optimization_barrier(jnp.mean(centered * centered, axis=-1, keepdims=True))
    inv_std = lax.rsqrt(row_var + epsilon)
    normed = centered * inv_std
    mixed_in = (normed * norm_gain + norm_bias).astype(jnp.bfloat16)
    pre_act = jnp.einsum('kp,bpc->bkc', w_first.astype(jnp.float32), mixed_in.astype(jnp.float32)) + b_first[None, :, None]
    gauss_cdf = 0.5 * (1.0 + lax.erf(pre_act * 0.7071067811865476))
    gauss_pdf = jnp.exp(-0.5 * pre_act * pre_act) * 0.3989422804014327
    activated = (pre_act * gauss_cdf).astype(jnp.bfloat16)
    upper = upstream.astype(jnp.float32)
    grad_act = jnp.einsum('pk,bpc->bkc', w_second.astype(jnp.float32), upper)
    grad_pre = (grad_act * (gauss_cdf + pre_act * gauss_pdf)).astype(jnp.bfloat16)
    pre_f = grad_pre.astype(jnp.float32)
    second_t = jnp.einsum('bkc,bpc->kp', activated.astype(jnp.float32), upper)
    first_w = jnp.einsum('bkc,bpc->kp', pre_f, mixed_in.astype(jnp.float32))
    first_b = lax.optimization_barrier(jnp.sum(pre_f, axis=(0, 2)))
    grad_mixed = jnp.einsum('kp,bkc->bpc', w_first.astype(jnp.float32), pre_f)
    gain_part = lax.optimization_barrier(jnp.sum(grad_mixed * normed, axis=(0, 1)))
    shift_part = lax.optimization_barrier(jnp.sum(grad_mixed, axis=(0, 1)))
    grad_normed = grad_mixed * norm_gain
    first_sum = lax.optimization_barrier(jnp.sum(grad_normed, axis=-1, keepdims=True))
    second_sum = lax.optimization_barrier(jnp.sum(grad_normed * normed, axis=-1, keepdims=True))
    grad_input = (upper + inv_std * (grad_normed - first_sum / D - normed * second_sum / D)).astype(jnp.bfloat16)
    return (grad_input, first_w, second_t, first_b, gain_part, shift_part)

def reference(inputs, norm_gain, norm_bias, w_first, b_first, w_second, upstream):
    blocks_in = inputs.reshape(N_DP, B_DEV, PATCHES, D)
    blocks_up = upstream.reshape(N_DP, B_DEV, PATCHES, D)

    def step(carry, pair):
        grad_in, first_w, second_t, first_b, gain_part, shift_part = block_pass(pair[0], pair[1], norm_gain, norm_bias, w_first, b_first, w_second)
        carry = (carry[0] + first_w, carry[1] + second_t, carry[2] + first_b, carry[3] + gain_part, carry[4] + shift_part)
        return (carry, grad_in)
    init = (jnp.zeros((TOKEN_HIDDEN, PATCHES), jnp.float32), jnp.zeros((TOKEN_HIDDEN, PATCHES), jnp.float32), jnp.zeros((TOKEN_HIDDEN,), jnp.float32), jnp.zeros((D,), jnp.float32), jnp.zeros((D,), jnp.float32))
    totals, grads = lax.scan(step, init, (blocks_in, blocks_up))
    scale = 1.0 / BATCH
    grad_input = grads.reshape(BATCH, PATCHES, D)
    return (grad_input, totals[0] * scale, (totals[1] * scale).T, totals[2] * scale, totals[3] * scale, totals[4] * scale)
```

```python
import functools

import jax
import jax.numpy as jnp
from jax import lax
from jax.experimental import pallas as pl
from jax.experimental.pallas import tpu as pltpu
from jax.sharding import PartitionSpec as P

epsilon = 1e-06
f32 = jnp.float32
bf16 = jnp.bfloat16
NT = (((1,), (1,)), ((), ()))
NN = (((1,), (0,)), ((), ()))


def round_up(n, m):
    return -(-n // m) * m


def divisor(n, most):
    return max(d for d in range(1, most + 1) if n % d == 0)


def column(ref, b, lanes):
    return pltpu.roll(ref[...], lax.rem(lanes - b, lanes), 1)[:, 0:1]


def stats_kernel(x_ref, out_ref, *, step_images, half):
    step = pl.program_id(0)
    patches, width = x_ref.shape[1:]

    @pl.when(step == 0)
    def _():
        out_ref[...] = jnp.zeros_like(out_ref)

    lane = lax.broadcasted_iota(jnp.int32, (patches, out_ref.shape[1]), 1)
    acc = out_ref[0:patches, :]
    for j in range(step_images):
        b = step * step_images + j
        x = x_ref[j].astype(f32)
        total = jnp.sum(x, axis=1, keepdims=True)
        d = x - total * (1.0 / width)
        spread = jnp.sum(d * d, axis=1, keepdims=True)
        acc = jnp.where(lane == b, total, acc)
        acc = jnp.where(lane == half + b, spread, acc)
    out_ref[0:patches, :] = acc


def main_kernel(*refs, step_images, half, chans, chunk):
    stat_refs = refs[:chans]
    (x_ref, up_ref, gain_ref, bias_ref, w1_ref, w2t_ref, w1t_ref,
     u_ref, sums_ref, mean_ref, rstd_ref, grads_ref, params_ref) = refs[chans:chans + 13]
    mixed_ref, upper_ref, gp_ref = refs[chans + 13:]
    step = pl.program_id(0)
    patches, width = x_ref.shape[1:]
    hidden, depth = w1_ref.shape
    lanes = sums_ref.shape[1]

    @pl.when(step == 0)
    def _():
        row = lax.broadcasted_iota(jnp.int32, mixed_ref.shape[1:], 0)
        ones = jnp.where((row >= patches) & (row < patches + 3), 1.0, 0.0).astype(bf16)
        for j in range(step_images):
            mixed_ref[j] = ones
            upper_ref[j] = jnp.zeros(upper_ref.shape[1:], bf16)
        stats = [r[...] for r in stat_refs]
        full = width * chans
        mean = sum(stats) * (1.0 / full)
        spread = sum(stats)
        spread = pltpu.roll(spread, half, 1)
        for s in stats:
            off = s * (1.0 / width) - mean
            spread = spread + width * (off * off)
        mean_ref[...] = mean
        rstd_ref[...] = lax.rsqrt(spread * (1.0 / full) + epsilon)
        sums_ref[...] = jnp.zeros_like(sums_ref)
        grads_ref[...] = jnp.zeros_like(grads_ref)
        params_ref[...] = jnp.zeros_like(params_ref)

    gain = gain_ref[...]
    bias = bias_ref[...]
    lane = lax.broadcasted_iota(jnp.int32, (patches, lanes), 1)
    sums = sums_ref[0:patches, :]
    for j in range(step_images):
        b = step * step_images + j
        mean = column(mean_ref, b, lanes)[0:patches]
        rstd = column(rstd_ref, b, lanes)[0:patches]
        normed = (x_ref[j].astype(f32) - mean) * rstd
        mixed_ref[j, 0:patches, :] = (normed * gain + bias).astype(bf16)
        upper_ref[j, 0:patches, :] = up_ref[j]
        for k in range(0, hidden, chunk):
            ks = pl.ds(k, chunk)
            pre = lax.dot_general(w1_ref[ks, :], mixed_ref[j], NN, preferred_element_type=f32)
            act = lax.dot_general(w2t_ref[ks, :], upper_ref[j], NN, preferred_element_type=f32)
            cdf = 0.5 + 0.5 * lax.erf(pre * 0.7071067811865476)
            pdf = jnp.exp2((pre * pre) * -0.7213475204444817) * 0.3989422804014327
            activated = (pre * cdf).astype(bf16)
            gp = (act * (cdf + pre * pdf)).astype(bf16)
            gp_ref[j, ks, :] = gp
            grads_ref[ks, 0:depth] += lax.dot_general(gp, mixed_ref[j], NT, preferred_element_type=f32)
            grads_ref[ks, depth:] += lax.dot_general(
                activated, upper_ref[j], NT, preferred_element_type=f32
            )
        gm = lax.dot_general(w1t_ref[...], gp_ref[j], NN, preferred_element_type=f32)[0:patches]
        gmn = gm * normed
        params_ref[0:1, :] += jnp.sum(gmn, axis=0, keepdims=True)
        params_ref[1:2, :] += jnp.sum(gm, axis=0, keepdims=True)
        gn = gm * gain
        first = jnp.sum(gn, axis=1, keepdims=True)
        second = jnp.sum(gmn * gain, axis=1, keepdims=True)
        sums = jnp.where(lane == b, first, sums)
        sums = jnp.where(lane == half + b, second, sums)
        u_ref[j] = (up_ref[j].astype(f32) + rstd * gn).astype(bf16)
    sums_ref[0:patches, :] = sums


def finish_kernel(*refs, step_images, half, chans, start):
    sum_refs = refs[:chans]
    mean_ref, rstd_ref, x_ref, u_ref, out_ref, add_ref, mul_ref = refs[chans:]
    step = pl.program_id(0)
    patches, width = x_ref.shape[1:]
    lanes = mean_ref.shape[1]

    @pl.when(step == 0)
    def _():
        first = sum(r[...] for r in sum_refs) * (1.0 / (width * chans))
        second = pltpu.roll(first, half, 1)
        rstd = rstd_ref[...]
        slope = rstd * rstd * second
        mul_ref[...] = -slope
        add_ref[...] = mean_ref[...] * slope - rstd * first

    for j in range(step_images):
        b = start + step * step_images + j
        add = column(add_ref, b, lanes)[0:patches]
        mul = column(mul_ref, b, lanes)[0:patches]
        out_ref[j] = (u_ref[j].astype(f32) + (add + mul * x_ref[j].astype(f32))).astype(bf16)


def swap(value, axis, bit, size):
    return lax.ppermute(value, axis, [(i, i ^ bit) for i in range(size)])


def peers(value, axis, size):
    return [value] + [
        lax.ppermute(value, axis, [(i, (i + d) % size) for i in range(size)]) for d in range(1, size)
    ]


def whole(shape):
    return pl.BlockSpec(shape, lambda i: (0,) * len(shape))


def per_device(inputs, norm_gain, norm_bias, w_first, b_first, w_second, upstream):
    images, patches, width = inputs.shape
    hidden = w_first.shape[0]
    chans = lax.axis_size("chan")
    ranks = lax.axis_size("dp")
    scale = 1.0 / (images * ranks)
    lanes = round_up(2 * images, 128)
    half = lanes // 2
    rows = round_up(patches, 8)
    depth = round_up(patches + 3, 128)
    tall = round_up(patches, 16)
    stat_shape = (rows, lanes)
    stat_type = jax.ShapeDtypeStruct(stat_shape, f32)
    params = pltpu.CompilerParams(
        dimension_semantics=("arbitrary",), vmem_limit_bytes=56 * 1024 * 1024
    )

    def image_spec(n, base=0):
        return pl.BlockSpec((n, patches, width), lambda i: (base + i, 0, 0))

    n_a = divisor(images, 8)
    stats = pl.pallas_call(
        functools.partial(stats_kernel, step_images=n_a, half=half),
        grid=(images // n_a,),
        in_specs=[image_spec(n_a)],
        out_specs=whole(stat_shape),
        out_shape=stat_type,
        compiler_params=params,
        name="row_stats",
    )(inputs)
    stats = peers(stats, "chan", chans)

    top = lax.reduce_precision(b_first, 8, 7)
    rest = b_first - top
    mid = lax.reduce_precision(rest, 8, 7)
    low = rest - mid
    split = jnp.stack([top, mid, low], axis=1).astype(bf16)
    w1 = jnp.pad(jnp.concatenate([w_first, split], axis=1), ((0, 0), (0, depth - patches - 3)))
    w2t = jnp.pad(w_second.T, ((0, 0), (0, depth - patches)))
    w1t = jnp.pad(w_first.T, ((0, tall - patches), (0, 0)))

    n_b = divisor(images, 2)
    chunk = hidden // 2
    u, sums, mean, rstd, grads, norm_grads = pl.pallas_call(
        functools.partial(main_kernel, step_images=n_b, half=half, chans=chans, chunk=chunk),
        grid=(images // n_b,),
        in_specs=[whole(stat_shape)] * chans
        + [image_spec(n_b)] * 2
        + [whole((1, width))] * 2
        + [whole((hidden, depth))] * 2
        + [whole((tall, hidden))],
        out_specs=[
            image_spec(n_b),
            whole(stat_shape),
            whole(stat_shape),
            whole(stat_shape),
            whole((hidden, 2 * depth)),
            whole((8, width)),
        ],
        out_shape=[
            jax.ShapeDtypeStruct(inputs.shape, bf16),
            stat_type,
            stat_type,
            stat_type,
            jax.ShapeDtypeStruct((hidden, 2 * depth), f32),
            jax.ShapeDtypeStruct((8, width), f32),
        ],
        scratch_shapes=[
            pltpu.VMEM((n_b, depth, width), bf16),
            pltpu.VMEM((n_b, depth, width), bf16),
            pltpu.VMEM((n_b, hidden, width), bf16),
        ],
        compiler_params=params,
        name="mix_backward",
    )(*stats, inputs, upstream, norm_gain[None], norm_bias[None], w1, w2t, w1t)

    sums = peers(sums, "chan", chans)

    pieces = 4 if images % 4 == 0 else 1
    part = images // pieces
    n_c = divisor(part, 6)
    out = u
    for piece in range(pieces):
        base = piece * part // n_c
        out = pl.pallas_call(
            functools.partial(
                finish_kernel, step_images=n_c, half=half, chans=chans, start=piece * part
            ),
            grid=(part // n_c,),
            in_specs=[whole(stat_shape)] * (chans + 2) + [image_spec(n_c, base)] * 2,
            out_specs=image_spec(n_c, base),
            out_shape=jax.ShapeDtypeStruct(inputs.shape, bf16),
            scratch_shapes=[pltpu.VMEM(stat_shape, f32)] * 2,
            input_output_aliases={chans + 3: 0},
            compiler_params=params,
            cost_estimate=pl.CostEstimate(
                flops=part * patches * width * 60,
                bytes_accessed=part * patches * width * 6,
                transcendentals=0,
            ),
            name=f"finish_{piece}",
        )(*sums, mean, rstd, inputs, out)

    me = lax.axis_index("dp")
    if ranks & (ranks - 1) == 0:
        bits = ranks.bit_length() - 1
        part_grads = grads.reshape((ranks, hidden // ranks, 2 * depth))
        norm_grads = norm_grads[0:2]
        for bit in range(bits):
            mine = (me >> bit) & 1
            pairs = part_grads.reshape((-1, 2) + part_grads.shape[1:])
            give = lax.dynamic_index_in_dim(pairs, 1 - mine, 1, keepdims=False)
            keep = lax.dynamic_index_in_dim(pairs, mine, 1, keepdims=False)
            part_grads = keep + swap(give, "dp", 1 << bit, ranks)
            norm_grads = norm_grads + swap(norm_grads, "dp", 1 << bit, ranks)
        owned = part_grads[0]
    else:
        owned = lax.psum_scatter(grads, "dp", scatter_dimension=0, tiled=True)
        norm_grads = lax.psum(norm_grads, "dp")
    owned = sum(peers(owned, "chan", chans)) * scale
    norm_grads = norm_grads * scale
    return (
        out,
        owned[:, 0:patches],
        owned[:, depth:depth + patches].T,
        owned[:, patches],
        norm_grads[0],
        norm_grads[1],
    )


def solution(mesh):
    in_specs = (P("dp", None, "chan"), P("chan"), P("chan"), P(), P(), P(), P("dp", None, "chan"))
    out_specs = (P("dp", None, "chan"), P("dp", None), P(None, "dp"), P("dp"), P("chan"), P("chan"))
    return jax.shard_map(
        per_device, mesh=mesh, in_specs=in_specs, out_specs=out_specs, check_vma=False
    )
```

```python
import functools

import jax
import jax.numpy as jnp
from jax import lax
from jax.experimental import pallas as pl
from jax.experimental.pallas import tpu as pltpu
from jax.sharding import PartitionSpec as P

epsilon = 1e-06
f32 = jnp.float32
bf16 = jnp.bfloat16
NT = (((1,), (1,)), ((), ()))
NN = (((1,), (0,)), ((), ()))


def round_up(n, m):
    return -(-n // m) * m


def divisor(n, most):
    return max(d for d in range(1, most + 1) if n % d == 0)


def column(ref, b, lanes):
    return pltpu.roll(ref[...], lax.rem(lanes - b, lanes), 1)[:, 0:1]


def stats_kernel(x_ref, out_ref, *, step_images, half):
    step = pl.program_id(0)
    patches, width = x_ref.shape[1:]

    @pl.when(step == 0)
    def _():
        out_ref[...] = jnp.zeros_like(out_ref)

    lane = lax.broadcasted_iota(jnp.int32, (patches, out_ref.shape[1]), 1)
    acc = out_ref[0:patches, :]
    for j in range(step_images):
        b = step * step_images + j
        x = x_ref[j].astype(f32)
        total = jnp.sum(x, axis=1, keepdims=True)
        d = x - total * (1.0 / width)
        spread = jnp.sum(d * d, axis=1, keepdims=True)
        acc = jnp.where(lane == b, total, acc)
        acc = jnp.where(lane == half + b, spread, acc)
    out_ref[0:patches, :] = acc


def main_kernel(*refs, step_images, half, chans, chunk):
    stat_refs = refs[:chans]
    (x_ref, up_ref, gain_ref, bias_ref, w1_ref, w2t_ref, w1t_ref,
     u_ref, sums_ref, mean_ref, rstd_ref, grads_ref, params_ref) = refs[chans:chans + 13]
    mixed_ref, upper_ref, gp_ref = refs[chans + 13:]
    step = pl.program_id(0)
    patches, width = x_ref.shape[1:]
    hidden, depth = w1_ref.shape
    lanes = sums_ref.shape[1]

    @pl.when(step == 0)
    def _():
        row = lax.broadcasted_iota(jnp.int32, mixed_ref.shape[1:], 0)
        ones = jnp.where((row >= patches) & (row < patches + 3), 1.0, 0.0).astype(bf16)
        for j in range(step_images):
            mixed_ref[j] = ones
            upper_ref[j] = jnp.zeros(upper_ref.shape[1:], bf16)
        stats = [r[...] for r in stat_refs]
        full = width * chans
        mean = sum(stats) * (1.0 / full)
        spread = sum(stats)
        spread = pltpu.roll(spread, half, 1)
        for s in stats:
            off = s * (1.0 / width) - mean
            spread = spread + width * (off * off)
        mean_ref[...] = mean
        rstd_ref[...] = lax.rsqrt(spread * (1.0 / full) + epsilon)
        sums_ref[...] = jnp.zeros_like(sums_ref)
        grads_ref[...] = jnp.zeros_like(grads_ref)
        params_ref[...] = jnp.zeros_like(params_ref)

    gain = gain_ref[...]
    bias = bias_ref[...]
    lane = lax.broadcasted_iota(jnp.int32, (patches, lanes), 1)
    sums = sums_ref[0:patches, :]
    for j in range(step_images):
        b = step * step_images + j
        mean = column(mean_ref, b, lanes)[0:patches]
        rstd = column(rstd_ref, b, lanes)[0:patches]
        normed = (x_ref[j].astype(f32) - mean) * rstd
        mixed_ref[j, 0:patches, :] = (normed * gain + bias).astype(bf16)
        upper_ref[j, 0:patches, :] = up_ref[j]
        for k in range(0, hidden, chunk):
            ks = pl.ds(k, chunk)
            pre = lax.dot_general(w1_ref[ks, :], mixed_ref[j], NN, preferred_element_type=f32)
            act = lax.dot_general(w2t_ref[ks, :], upper_ref[j], NN, preferred_element_type=f32)
            cdf = 0.5 + 0.5 * lax.erf(pre * 0.7071067811865476)
            pdf = jnp.exp2((pre * pre) * -0.7213475204444817) * 0.3989422804014327
            activated = (pre * cdf).astype(bf16)
            gp = (act * (cdf + pre * pdf)).astype(bf16)
            gp_ref[j, ks, :] = gp
            grads_ref[ks, 0:depth] += lax.dot_general(gp, mixed_ref[j], NT, preferred_element_type=f32)
            grads_ref[ks, depth:] += lax.dot_general(
                activated, upper_ref[j], NT, preferred_element_type=f32
            )
        gm = lax.dot_general(w1t_ref[...], gp_ref[j], NN, preferred_element_type=f32)[0:patches]
        gmn = gm * normed
        params_ref[0:1, :] += jnp.sum(gmn, axis=0, keepdims=True)
        params_ref[1:2, :] += jnp.sum(gm, axis=0, keepdims=True)
        gn = gm * gain
        first = jnp.sum(gn, axis=1, keepdims=True)
        second = jnp.sum(gmn * gain, axis=1, keepdims=True)
        sums = jnp.where(lane == b, first, sums)
        sums = jnp.where(lane == half + b, second, sums)
        u_ref[j] = (up_ref[j].astype(f32) + rstd * gn).astype(bf16)
    sums_ref[0:patches, :] = sums


def finish_kernel(*refs, step_images, half, chans, start):
    sum_refs = refs[:chans]
    mean_ref, rstd_ref, x_ref, u_ref, out_ref, add_ref, mul_ref = refs[chans:]
    step = pl.program_id(0)
    patches, width = x_ref.shape[1:]
    lanes = mean_ref.shape[1]

    @pl.when(step == 0)
    def _():
        first = sum(r[...] for r in sum_refs) * (1.0 / (width * chans))
        second = pltpu.roll(first, half, 1)
        rstd = rstd_ref[...]
        slope = rstd * rstd * second
        mul_ref[...] = -slope
        add_ref[...] = mean_ref[...] * slope - rstd * first

    for j in range(step_images):
        b = start + step * step_images + j
        add = column(add_ref, b, lanes)[0:patches]
        mul = column(mul_ref, b, lanes)[0:patches]
        out_ref[j] = (u_ref[j].astype(f32) + (add + mul * x_ref[j].astype(f32))).astype(bf16)


def swap(value, axis, bit, size):
    return lax.ppermute(value, axis, [(i, i ^ bit) for i in range(size)])


def peers(value, axis, size):
    return [value] + [
        lax.ppermute(value, axis, [(i, (i + d) % size) for i in range(size)]) for d in range(1, size)
    ]


def whole(shape):
    return pl.BlockSpec(shape, lambda i: (0,) * len(shape))


def per_device(inputs, norm_gain, norm_bias, w_first, b_first, w_second, upstream):
    images, patches, width = inputs.shape
    hidden = w_first.shape[0]
    chans = lax.axis_size("chan")
    ranks = lax.axis_size("dp")
    scale = 1.0 / (images * ranks)
    lanes = round_up(2 * images, 128)
    half = lanes // 2
    rows = round_up(patches, 8)
    depth = round_up(patches + 3, 128)
    tall = round_up(patches, 16)
    stat_shape = (rows, lanes)
    stat_type = jax.ShapeDtypeStruct(stat_shape, f32)
    params = pltpu.CompilerParams(
        dimension_semantics=("arbitrary",), vmem_limit_bytes=56 * 1024 * 1024
    )

    def image_spec(n, base=0):
        return pl.BlockSpec((n, patches, width), lambda i: (base + i, 0, 0))

    n_a = divisor(images, 8)
    stats = pl.pallas_call(
        functools.partial(stats_kernel, step_images=n_a, half=half),
        grid=(images // n_a,),
        in_specs=[image_spec(n_a)],
        out_specs=whole(stat_shape),
        out_shape=stat_type,
        compiler_params=params,
        name="row_stats",
    )(inputs)
    stats = peers(stats, "chan", chans)

    top = lax.reduce_precision(b_first, 8, 7)
    rest = b_first - top
    mid = lax.reduce_precision(rest, 8, 7)
    low = rest - mid
    split = jnp.stack([top, mid, low], axis=1).astype(bf16)
    w1 = jnp.pad(jnp.concatenate([w_first, split], axis=1), ((0, 0), (0, depth - patches - 3)))
    w2t = jnp.pad(w_second.T, ((0, 0), (0, depth - patches)))
    w1t = jnp.pad(w_first.T, ((0, tall - patches), (0, 0)))

    n_b = divisor(images, 2)
    chunk = hidden // 2
    u, sums, mean, rstd, grads, norm_grads = pl.pallas_call(
        functools.partial(main_kernel, step_images=n_b, half=half, chans=chans, chunk=chunk),
        grid=(images // n_b,),
        in_specs=[whole(stat_shape)] * chans
        + [image_spec(n_b)] * 2
        + [whole((1, width))] * 2
        + [whole((hidden, depth))] * 2
        + [whole((tall, hidden))],
        out_specs=[
            image_spec(n_b),
            whole(stat_shape),
            whole(stat_shape),
            whole(stat_shape),
            whole((hidden, 2 * depth)),
            whole((8, width)),
        ],
        out_shape=[
            jax.ShapeDtypeStruct(inputs.shape, bf16),
            stat_type,
            stat_type,
            stat_type,
            jax.ShapeDtypeStruct((hidden, 2 * depth), f32),
            jax.ShapeDtypeStruct((8, width), f32),
        ],
        scratch_shapes=[
            pltpu.VMEM((n_b, depth, width), bf16),
            pltpu.VMEM((n_b, depth, width), bf16),
            pltpu.VMEM((n_b, hidden, width), bf16),
        ],
        compiler_params=params,
        name="mix_backward",
    )(*stats, inputs, upstream, norm_gain[None], norm_bias[None], w1, w2t, w1t)

    sums = peers(sums, "chan", chans)

    held = lax.optimization_barrier((grads, norm_grads, *sums))
    grads, norm_grads, sums = held[0], held[1][0:2], list(held[2:])
    paired = ranks & (ranks - 1) == 0
    bits = ranks.bit_length() - 1 if paired else 1
    pieces = divisor(images, bits)
    part = images // pieces
    n_c = divisor(part, 6)

    def finish(piece, out):
        base = piece * part // n_c
        return pl.pallas_call(
            functools.partial(
                finish_kernel, step_images=n_c, half=half, chans=chans, start=piece * part
            ),
            grid=(part // n_c,),
            in_specs=[whole(stat_shape)] * (chans + 2) + [image_spec(n_c, base)] * 2,
            out_specs=image_spec(n_c, base),
            out_shape=jax.ShapeDtypeStruct(inputs.shape, bf16),
            scratch_shapes=[pltpu.VMEM(stat_shape, f32)] * 2,
            input_output_aliases={chans + 3: 0},
            compiler_params=params,
            cost_estimate=pl.CostEstimate(
                flops=part * patches * width * 200,
                bytes_accessed=part * patches * width * 6,
                transcendentals=0,
            ),
            name=f"finish_{piece}",
        )(*sums, mean, rstd, inputs, out)

    me = lax.axis_index("dp")
    out = u
    if paired:
        part_grads = grads.reshape((ranks, hidden // ranks, 2 * depth))
        for r in range(bits):
            mine = (me >> r) & 1
            pairs = part_grads.reshape((-1, 2) + part_grads.shape[1:])
            give = lax.dynamic_index_in_dim(pairs, 1 - mine, 1, keepdims=False)
            keep = lax.dynamic_index_in_dim(pairs, mine, 1, keepdims=False)
            give = swap(give, "dp", 1 << r, ranks)
            other = swap(norm_grads, "dp", 1 << r, ranks)
            if r < pieces:
                out = finish(r, out)
                give, other, out = lax.optimization_barrier((give, other, out))
            part_grads = keep + give
            norm_grads = norm_grads + other
        owned = part_grads[0]
    else:
        out = finish(0, out)
        owned = lax.psum_scatter(grads, "dp", scatter_dimension=0, tiled=True)
        norm_grads = lax.psum(norm_grads, "dp")
    owned = sum(peers(owned, "chan", chans)) * scale
    norm_grads = norm_grads * scale
    return (
        out,
        owned[:, 0:patches],
        owned[:, depth:depth + patches].T,
        owned[:, patches],
        norm_grads[0],
        norm_grads[1],
    )


def solution(mesh):
    in_specs = (P("dp", None, "chan"), P("chan"), P("chan"), P(), P(), P(), P("dp", None, "chan"))
    out_specs = (P("dp", None, "chan"), P("dp", None), P(None, "dp"), P("dp"), P("chan"), P("chan"))
    return jax.shard_map(
        per_device, mesh=mesh, in_specs=in_specs, out_specs=out_specs, check_vma=False
    )
```
